16 devices in a mesh: cp: 2 (over z), fsdp: 8 (over y, x, core).
Axes of the slice: x: 2, y: 2, z: 2, core: 2. Of those that a mesh axis runs over, the one named last changes fastest.
Arguments:
- hidden: bfloat16 [64, 256, 4096], P('fsdp', 'cp')
- tok_pos: int32 [64, 256], P('fsdp', 'cp')
- grad_out: bfloat16 [64, 256, 4096], P('fsdp', 'cp')
- norm_gain: float32 [4096], P(('fsdp', 'cp'))
- w_query: bfloat16 [4096, 4096], P(('fsdp', 'cp'))
- w_key: bfloat16 [4096, 1024], P(('fsdp', 'cp'))
- w_value: bfloat16 [4096, 1024], P(('fsdp', 'cp'))
- w_out: bfloat16 [4096, 4096], P(('fsdp', 'cp'))
Outputs:
- output 1: bfloat16 [64, 256, 4096], P('fsdp', 'cp')
- output 2: bfloat16 [64, 256, 4096], P('fsdp', 'cp')
- output 3: float32 [4096, 4096], P(('fsdp', 'cp'))
- output 4: float32 [4096, 1024], P(('fsdp', 'cp'))
- output 5: float32 [4096, 1024], P(('fsdp', 'cp'))
- output 6: float32 [4096, 4096], P(('fsdp', 'cp'))
- output 7: float32 [4096], P(('fsdp', 'cp'))
All inputs are finite; a program needn't handle non-finite values.
Results may differ from the reference program's by a relative error of at most 0.00717624.
Values are sent between devices in bfloat16 or wider.
A program may use at most 1 GiB of HBM per device.

```python
import jax
import jax.numpy as jnp
from jax import lax

SEQS_TOTAL = 64
SEQ_LEN = 256
MODEL_DIM = 4096
NUM_HEADS = 32
NUM_KV_HEADS = 8
HEAD_DIM = 128
Q_BLOCK = 32
ROPE_THETA = 1000000.0
RMS_EPS = 1e-5
NEG_BIG = -1e30
SCALE = HEAD_DIM ** -0.5
GROUP_SIZE = NUM_HEADS // NUM_KV_HEADS
N_QBLOCKS = SEQ_LEN // Q_BLOCK


def setup_inputs(seed: int = 0) -> dict:
    rand_keys = jax.random.split(jax.random.key(seed), 8)
    q_cols = NUM_HEADS * HEAD_DIM
    kv_cols = NUM_KV_HEADS * HEAD_DIM
    in_scale = MODEL_DIM ** -0.5
    hidden = jax.random.normal(rand_keys[0], (SEQS_TOTAL, SEQ_LEN, MODEL_DIM), jnp.float32)
    base_pos = jnp.broadcast_to(jnp.arange(SEQ_LEN, dtype=jnp.int32), (SEQS_TOTAL, SEQ_LEN))
    tok_pos = jax.random.permutation(rand_keys[1], base_pos, axis=1, independent=True)
    grad_out = jax.random.normal(rand_keys[2], (SEQS_TOTAL, SEQ_LEN, MODEL_DIM), jnp.float32)
    norm_gain = jax.random.uniform(rand_keys[3], (MODEL_DIM,), jnp.float32, 0.5, 1.5)
    w_query = jax.random.normal(rand_keys[4], (MODEL_DIM, q_cols), jnp.float32) * in_scale
    w_key = jax.random.normal(rand_keys[5], (MODEL_DIM, kv_cols), jnp.float32) * in_scale
    w_value = jax.random.normal(rand_keys[6], (MODEL_DIM, kv_cols), jnp.float32) * in_scale
    w_out = jax.random.normal(rand_keys[7], (q_cols, MODEL_DIM), jnp.float32) * q_cols ** -0.5
    return {'hidden': hidden.astype(jnp.bfloat16), 'tok_pos': tok_pos, 'grad_out': grad_out.astype(jnp.bfloat16), 'norm_gain': norm_gain, 'w_query': w_query.astype(jnp.bfloat16), 'w_key': w_key.astype(jnp.bfloat16), 'w_value': w_value.astype(jnp.bfloat16), 'w_out': w_out.astype(jnp.bfloat16)}


def rope_tables(positions):
    half_dim = HEAD_DIM // 2
    inv_freq = ROPE_THETA ** (-jnp.arange(half_dim, dtype=jnp.float32) / half_dim)
    angles = positions.astype(jnp.float32)[..., None] * inv_freq
    return jnp.cos(angles)[..., None, :], jnp.sin(angles)[..., None, :]


def rope_apply(values, cos_tab, sin_tab):
    half_dim = HEAD_DIM // 2
    first_half = values[..., :half_dim]
    second_half = values[..., half_dim:]
    return jnp.concatenate([first_half * cos_tab - second_half * sin_tab, second_half * cos_tab + first_half * sin_tab], axis=-1)


def rope_transpose(values, cos_tab, sin_tab):
    half_dim = HEAD_DIM // 2
    first_half = values[..., :half_dim]
    second_half = values[..., half_dim:]
    return jnp.concatenate([first_half * cos_tab + second_half * sin_tab, second_half * cos_tab - first_half * sin_tab], axis=-1)


def seq_pass(hidden, tok_pos, grad_out, norm_gain, w_query, w_key, w_value, w_out):
    x_f32 = hidden.astype(jnp.float32)
    inv_rms = lax.rsqrt(jnp.mean(x_f32 * x_f32, axis=-1) + RMS_EPS)
    x_hat = x_f32 * inv_rms[:, None]
    normed = (x_hat * norm_gain).astype(jnp.bfloat16)
    cos_tab, sin_tab = rope_tables(tok_pos)
    q_lin = jnp.dot(normed, w_query, preferred_element_type=jnp.float32).reshape(SEQ_LEN, NUM_HEADS, HEAD_DIM)
    k_lin = jnp.dot(normed, w_key, preferred_element_type=jnp.float32).reshape(SEQ_LEN, NUM_KV_HEADS, HEAD_DIM)
    q_rot = rope_apply(q_lin, cos_tab, sin_tab).astype(jnp.bfloat16)
    k_rot = rope_apply(k_lin, cos_tab, sin_tab).astype(jnp.bfloat16)
    v_val = jnp.dot(normed, w_value, preferred_element_type=jnp.float32).astype(jnp.bfloat16).reshape(SEQ_LEN, NUM_KV_HEADS, HEAD_DIM)
    k_f32 = k_rot.astype(jnp.float32)
    v_f32 = v_val.astype(jnp.float32)
    q_blocks = q_rot.reshape(N_QBLOCKS, Q_BLOCK, NUM_KV_HEADS, GROUP_SIZE, HEAD_DIM)
    pos_blocks = tok_pos.reshape(N_QBLOCKS, Q_BLOCK)

    def block_scores(q_blk, q_pos):
        scores = jnp.einsum('ikgd,jkd->kigj', q_blk.astype(jnp.float32), k_f32) * SCALE
        visible = tok_pos[None, None, None, :] <= q_pos[None, :, None, None]
        return jnp.where(visible, scores, NEG_BIG), visible

    def fwd_block(blk_args):
        q_blk, q_pos = blk_args
        scores, visible = block_scores(q_blk, q_pos)
        row_max = jnp.max(scores, axis=-1)
        att_probs = jnp.where(visible, jnp.exp(scores - row_max[..., None]), 0.0)
        row_sum = jnp.sum(att_probs, axis=-1)
        out_blk = jnp.einsum('kigj,jkd->ikgd', att_probs.astype(jnp.bfloat16).astype(jnp.float32), v_f32)
        out_blk = out_blk / jnp.transpose(row_sum, (1, 0, 2))[..., None]
        return out_blk.astype(jnp.bfloat16), row_max + jnp.log(row_sum)

    attn_out, log_sum = lax.map(fwd_block, (q_blocks, pos_blocks))
    attn_flat = attn_out.reshape(SEQ_LEN, NUM_HEADS * HEAD_DIM)
    result = (x_f32 + jnp.dot(attn_flat, w_out, preferred_element_type=jnp.float32)).astype(jnp.bfloat16)
    grad_w_out = jnp.dot(attn_flat.T, grad_out, preferred_element_type=jnp.float32)
    grad_attn = jnp.dot(grad_out, w_out.T, preferred_element_type=jnp.float32).astype(jnp.bfloat16)
    gout_blocks = grad_attn.reshape(N_QBLOCKS, Q_BLOCK, NUM_KV_HEADS, GROUP_SIZE, HEAD_DIM)
    row_delta = jnp.einsum('nikgd,nikgd->nkig', gout_blocks.astype(jnp.float32), attn_out.astype(jnp.float32))

    def bwd_block(kv_grads, blk_args):
        grad_k, grad_v = kv_grads
        q_blk, q_pos, gout_blk, lse_blk, delta_blk = blk_args
        scores, visible = block_scores(q_blk, q_pos)
        att_probs = jnp.where(visible, jnp.exp(scores - lse_blk[..., None]), 0.0)
        gout_f32 = gout_blk.astype(jnp.float32)
        grad_v = grad_v + jnp.einsum('kigj,ikgd->jkd', att_probs.astype(jnp.bfloat16).astype(jnp.float32), gout_f32)
        grad_probs = jnp.einsum('ikgd,jkd->kigj', gout_f32, v_f32)
        grad_scores = (att_probs * (grad_probs - delta_blk[..., None])).astype(jnp.bfloat16).astype(jnp.float32)
        grad_q = jnp.einsum('kigj,jkd->ikgd', grad_scores, k_f32)
        grad_k = grad_k + jnp.einsum('kigj,ikgd->jkd', grad_scores, q_blk.astype(jnp.float32))
        return (grad_k, grad_v), grad_q

    zero_kv = jnp.zeros((SEQ_LEN, NUM_KV_HEADS, HEAD_DIM), jnp.float32)
    kv_grads, grad_q = lax.scan(bwd_block, (zero_kv, zero_kv), (q_blocks, pos_blocks, gout_blocks, log_sum, row_delta))
    dq_pre = rope_transpose(grad_q.reshape(SEQ_LEN, NUM_HEADS, HEAD_DIM) * SCALE, cos_tab, sin_tab).astype(jnp.bfloat16).reshape(SEQ_LEN, NUM_HEADS * HEAD_DIM)
    dk_pre = rope_transpose(kv_grads[0] * SCALE, cos_tab, sin_tab).astype(jnp.bfloat16).reshape(SEQ_LEN, NUM_KV_HEADS * HEAD_DIM)
    dv_pre = kv_grads[1].astype(jnp.bfloat16).reshape(SEQ_LEN, NUM_KV_HEADS * HEAD_DIM)
    grad_w_query = jnp.dot(normed.T, dq_pre, preferred_element_type=jnp.float32)
    grad_w_key = jnp.dot(normed.T, dk_pre, preferred_element_type=jnp.float32)
    grad_w_value = jnp.dot(normed.T, dv_pre, preferred_element_type=jnp.float32)
    grad_normed = (jnp.dot(dq_pre, w_query.T, preferred_element_type=jnp.float32) + jnp.dot(dk_pre, w_key.T, preferred_element_type=jnp.float32) + jnp.dot(dv_pre, w_value.T, preferred_element_type=jnp.float32))
    grad_xhat = grad_normed * norm_gain
    grad_gain = jnp.sum(grad_normed * x_hat, axis=0)
    grad_x = inv_rms[:, None] * (grad_xhat - x_hat * jnp.mean(grad_xhat * x_hat, axis=-1, keepdims=True))
    grad_hidden = (grad_out.astype(jnp.float32) + grad_x).astype(jnp.bfloat16)
    return result, grad_hidden, (grad_w_query, grad_w_key, grad_w_value, grad_w_out, grad_gain)


def reference(hidden, tok_pos, grad_out, norm_gain, w_query, w_key, w_value, w_out):
    def per_seq(totals, seq_args):
        result, grad_hidden, seq_grads = seq_pass(seq_args[0], seq_args[1], seq_args[2], norm_gain, w_query, w_key, w_value, w_out)
        return jax.tree.map(jnp.add, totals, seq_grads), (result, grad_hidden)

    init_totals = (jnp.zeros(w_query.shape, jnp.float32), jnp.zeros(w_key.shape, jnp.float32), jnp.zeros(w_value.shape, jnp.float32), jnp.zeros(w_out.shape, jnp.float32), jnp.zeros(norm_gain.shape, jnp.float32))
    totals, seq_outs = lax.scan(per_seq, init_totals, (hidden, tok_pos, grad_out))
    return seq_outs[0], seq_outs[1], totals[0], totals[1], totals[2], totals[3], totals[4]
```

```python
import functools

import jax
import jax.numpy as jnp
from jax import lax
from jax.experimental import pallas as pl
from jax.experimental.pallas import tpu as pltpu
from jax.sharding import PartitionSpec as P


HEAD_DIM = 128
ROPE_THETA = 1000000.0
RMS_EPS = 1e-5
NEG_BIG = -1e30
SCALE = HEAD_DIM ** -0.5
ALL_AXES = ('fsdp', 'cp')
NT = (((1,), (1,)), ((), ()))
TN = (((0,), (0,)), ((), ()))
BLK = 256


def rotate(val, cos_tab, sin_tab):
    return val * cos_tab + pltpu.roll(val, 64, 1) * sin_tab


def rotate_back(val, cos_tab, sin_tab):
    return val * cos_tab - pltpu.roll(val, 64, 1) * sin_tab


def rope_kv_kernel(kv_ref, cos_ref, sin_ref, out_ref):
    cos_tab, sin_tab = cos_ref[...], sin_ref[...]
    width = kv_ref.shape[1]
    for col in range(0, width // 2, HEAD_DIM):
        out_ref[:, col:col + HEAD_DIM] = rotate(kv_ref[:, col:col + HEAD_DIM], cos_tab, sin_tab).astype(jnp.bfloat16)
    out_ref[:, width // 2:] = kv_ref[:, width // 2:].astype(jnp.bfloat16)


def rope_kv(kv_lin, cos_tab, sin_tab):
    tokens, width = kv_lin.shape
    rows = 128
    return pl.pallas_call(
        rope_kv_kernel,
        grid=(tokens // rows,),
        in_specs=[pl.BlockSpec((rows, width), lambda i: (i, 0)), pl.BlockSpec((rows, HEAD_DIM), lambda i: (i, 0)), pl.BlockSpec((rows, HEAD_DIM), lambda i: (i, 0))],
        out_specs=pl.BlockSpec((rows, width), lambda i: (i, 0)),
        out_shape=jax.ShapeDtypeStruct((tokens, width), jnp.bfloat16),
        cost_estimate=pl.CostEstimate(flops=tokens * width * 1000, bytes_accessed=tokens * width * 6, transcendentals=0),
        name="rope_kv",
    )(kv_lin, cos_tab, sin_tab)


def finish_dkv_kernel(dk_ref, dkr_ref, dv_ref, dvr_ref, cos_ref, sin_ref, out_ref):
    cos_tab, sin_tab = cos_ref[...], sin_ref[...]
    width = dk_ref.shape[1]
    for col in range(0, width, HEAD_DIM):
        cols = slice(col, col + HEAD_DIM)
        out_ref[:, cols] = rotate_back((dk_ref[:, cols] + dkr_ref[:, cols]) * SCALE, cos_tab, sin_tab).astype(jnp.bfloat16)
    out_ref[:, width:] = (dv_ref[...] + dvr_ref[...]).astype(jnp.bfloat16)


def finish_dkv(dk_own, dk_recv, dv_own, dv_recv, cos_tab, sin_tab):
    tokens, width = dk_own.shape
    rows = 128
    part = pl.BlockSpec((rows, width), lambda i: (i, 0))
    tab = pl.BlockSpec((rows, HEAD_DIM), lambda i: (i, 0))
    return pl.pallas_call(
        finish_dkv_kernel,
        grid=(tokens // rows,),
        in_specs=[part, part, part, part, tab, tab],
        out_specs=pl.BlockSpec((rows, 2 * width), lambda i: (i, 0)),
        out_shape=jax.ShapeDtypeStruct((tokens, 2 * width), jnp.bfloat16),
        cost_estimate=pl.CostEstimate(flops=tokens * width * 2000, bytes_accessed=tokens * width * 20, transcendentals=0),
        name="finish_dkv",
    )(dk_own, dk_recv, dv_own, dv_recv, cos_tab, sin_tab)


def prep_kernel(x_ref, gain_ref, out_ref, out_t_ref):
    x_f32 = x_ref[...].astype(jnp.float32)
    inv_rms = lax.rsqrt(jnp.mean(x_f32 * x_f32, axis=-1, keepdims=True) + RMS_EPS)
    for col in range(0, x_ref.shape[1], 128):
        cols = slice(col, col + 128)
        normed = (x_ref[:, cols].astype(jnp.float32) * inv_rms * gain_ref[:, cols]).astype(jnp.bfloat16)
        out_ref[:, cols] = normed
        out_t_ref[cols, :] = normed.astype(jnp.float32).T.astype(jnp.bfloat16)


def prep(x_bf, gain):
    tokens, dim = x_bf.shape
    rows = 128
    return pl.pallas_call(
        prep_kernel,
        grid=(tokens // rows,),
        in_specs=[pl.BlockSpec((rows, dim), lambda i: (i, 0)), pl.BlockSpec((1, dim), lambda i: (0, 0))],
        out_specs=[pl.BlockSpec((rows, dim), lambda i: (i, 0)), pl.BlockSpec((dim, rows), lambda i: (0, i))],
        out_shape=[jax.ShapeDtypeStruct((tokens, dim), jnp.bfloat16), jax.ShapeDtypeStruct((dim, tokens), jnp.bfloat16)],
        cost_estimate=pl.CostEstimate(flops=tokens * dim * 1000, bytes_accessed=tokens * dim * 6, transcendentals=0),
        name="prep",
    )(x_bf, gain)


def epilogue_kernel(dr_ref, x_ref, dy_ref, gain_ref, out_ref, gain_out_ref):
    x_f32 = x_ref[...].astype(jnp.float32)
    inv_rms = lax.rsqrt(jnp.mean(x_f32 * x_f32, axis=-1, keepdims=True) + RMS_EPS)
    x_hat = x_f32 * inv_rms
    grad_normed = dr_ref[...]
    gain_part = jnp.sum(grad_normed * x_hat, axis=0, keepdims=True)

    @pl.when(pl.program_id(0) == 0)
    def _():
        gain_out_ref[...] = gain_part

    @pl.when(pl.program_id(0) > 0)
    def _():
        gain_out_ref[...] += gain_part

    grad_xhat = grad_normed * gain_ref[...]
    grad_x = inv_rms * (grad_xhat - x_hat * jnp.mean(grad_xhat * x_hat, axis=-1, keepdims=True))
    out_ref[...] = (dy_ref[...].astype(jnp.float32) + grad_x).astype(jnp.bfloat16)


def epilogue(grad_normed, x_bf, dy, gain):
    tokens, dim = x_bf.shape
    rows = 64
    full = pl.BlockSpec((rows, dim), lambda i: (i, 0))
    vec = pl.BlockSpec((1, dim), lambda i: (0, 0))
    return pl.pallas_call(
        epilogue_kernel,
        grid=(tokens // rows,),
        in_specs=[full, full, full, vec],
        out_specs=[full, vec],
        out_shape=[jax.ShapeDtypeStruct((tokens, dim), jnp.bfloat16), jax.ShapeDtypeStruct((1, dim), jnp.float32)],
        cost_estimate=pl.CostEstimate(flops=tokens * dim * 1000, bytes_accessed=tokens * dim * 10, transcendentals=0),
        name="epilogue",
    )(grad_normed, x_bf, dy, gain)


def scores_t(keys, queries, mask_t, heads):
    st = lax.dot_general(keys, queries, NT, preferred_element_type=jnp.float32) * SCALE
    return jnp.where(jnp.concatenate([mask_t] * heads, axis=1), st, NEG_BIG)


def attn_fwd_kernel(heads, q_ref, ko_ref, vo_ref, kp_ref, vp_ref, cos_ref, sin_ref, qpos_ref, kpos_ref, o_ref, ot_ref, qr_ref):
    cos_tab, sin_tab = cos_ref[...], sin_ref[...]
    mask_t = kpos_ref[0] <= qpos_ref[0]
    groups = ko_ref.shape[1] // HEAD_DIM
    for grp in range(groups):
        kcols = slice(grp * HEAD_DIM, (grp + 1) * HEAD_DIM)
        keys = jnp.concatenate([ko_ref[:, kcols], kp_ref[:, kcols]], axis=0)
        vals = jnp.concatenate([vo_ref[:, kcols], vp_ref[:, kcols]], axis=0)
        rot = []
        for head in range(heads):
            col = (grp * heads + head) * HEAD_DIM
            q_rot = rotate(q_ref[:, col:col + HEAD_DIM], cos_tab, sin_tab).astype(jnp.bfloat16)
            qr_ref[:, col:col + HEAD_DIM] = q_rot
            rot.append(q_rot)
        queries = jnp.concatenate(rot, axis=0)
        st = scores_t(keys, queries, mask_t, heads)
        row_max = jnp.max(st, axis=0, keepdims=True)
        probs = jnp.exp(st - row_max)
        row_sum = jnp.sum(probs, axis=0, keepdims=True)
        out_t = lax.dot_general(vals, probs.astype(jnp.bfloat16), TN, preferred_element_type=jnp.float32) / row_sum
        for head in range(heads):
            col = (grp * heads + head) * HEAD_DIM
            part = out_t[:, head * 128:(head + 1) * 128]
            ot_ref[col:col + HEAD_DIM, :] = part.astype(jnp.bfloat16)
            o_ref[:, col:col + HEAD_DIM] = part.T.astype(jnp.bfloat16)


def attn_specs(heads, groups, kv_blocks):
    rows = 128
    q_spec = pl.BlockSpec((rows, groups * heads * HEAD_DIM), lambda b, g: (b, g))
    k_spec = pl.BlockSpec((rows, groups * HEAD_DIM), lambda b, g: (b, g))
    v_spec = pl.BlockSpec((rows, groups * HEAD_DIM), lambda b, g: (b, kv_blocks + g))
    tab = pl.BlockSpec((rows, HEAD_DIM), lambda b, g: (b, 0))
    qpos = pl.BlockSpec((1, 1, rows), lambda b, g: (b, 0, 0))
    kpos = pl.BlockSpec((1, 2 * rows, 1), lambda b, g: (b, 0, 0))
    return q_spec, k_spec, v_spec, tab, qpos, kpos


def attn_fwd(q_lin, kv_own, kv_prt, cos_tab, sin_tab, qpos, kpos, n_seq):
    tokens, q_cols = q_lin.shape
    kv_cols = kv_own.shape[1] // 2
    heads = q_cols // kv_cols
    groups = 2
    kv_blocks = kv_cols // HEAD_DIM // groups
    q_spec, k_spec, v_spec, tab, qpos_spec, kpos_spec = attn_specs(heads, groups, kv_blocks)
    rows = tokens // n_seq
    return pl.pallas_call(
        functools.partial(attn_fwd_kernel, heads),
        grid=(n_seq, kv_blocks),
        in_specs=[q_spec, k_spec, v_spec, k_spec, v_spec, tab, tab, qpos_spec, kpos_spec],
        out_specs=[q_spec, pl.BlockSpec((groups * heads * HEAD_DIM, rows), lambda b, g: (g, b)), q_spec],
        out_shape=[jax.ShapeDtypeStruct((tokens, q_cols), jnp.bfloat16), jax.ShapeDtypeStruct((q_cols, tokens), jnp.bfloat16), jax.ShapeDtypeStruct((tokens, q_cols), jnp.bfloat16)],
        cost_estimate=pl.CostEstimate(flops=30 * 10 ** 9, bytes_accessed=tokens * q_cols * 10, transcendentals=tokens * q_cols * 2),
        compiler_params=pltpu.CompilerParams(dimension_semantics=("arbitrary", "arbitrary")),
        name="attn_fwd",
    )(q_lin, kv_own, kv_own, kv_prt, kv_prt, cos_tab, sin_tab, qpos, kpos)


def attn_bwd_kernel(heads, q_ref, ko_ref, vo_ref, kp_ref, vp_ref, do_ref, o_ref, cos_ref, sin_ref, qpos_ref, kpos_ref, dq_ref, dko_ref, dvo_ref, dkp_ref, dvp_ref):
    cos_tab, sin_tab = cos_ref[...], sin_ref[...]
    mask_t = kpos_ref[0] <= qpos_ref[0]
    groups = ko_ref.shape[1] // HEAD_DIM
    rows = q_ref.shape[0]
    for grp in range(groups):
        kcols = slice(grp * HEAD_DIM, (grp + 1) * HEAD_DIM)
        keys = jnp.concatenate([ko_ref[:, kcols], kp_ref[:, kcols]], axis=0)
        vals = jnp.concatenate([vo_ref[:, kcols], vp_ref[:, kcols]], axis=0)
        cols = [slice((grp * heads + head) * HEAD_DIM, (grp * heads + head + 1) * HEAD_DIM) for head in range(heads)]
        queries = jnp.concatenate([q_ref[:, c] for c in cols], axis=0)
        gout = jnp.concatenate([do_ref[:, c] for c in cols], axis=0)
        delta = jnp.concatenate([jnp.sum((do_ref[:, c].astype(jnp.float32) * o_ref[:, c].astype(jnp.float32)).T, axis=0, keepdims=True) for c in cols], axis=1)
        st = scores_t(keys, queries, mask_t, heads)
        row_max = jnp.max(st, axis=0, keepdims=True)
        probs = jnp.exp(st - row_max)
        probs = probs * (1.0 / jnp.sum(probs, axis=0, keepdims=True))
        grad_p = lax.dot_general(vals, gout, NT, preferred_element_type=jnp.float32)
        grad_s = (probs * (grad_p - delta)).astype(jnp.bfloat16)
        grad_v = jnp.dot(probs.astype(jnp.bfloat16), gout, preferred_element_type=jnp.float32)
        grad_k = jnp.dot(grad_s, queries, preferred_element_type=jnp.float32)
        grad_qt = lax.dot_general(keys, grad_s, TN, preferred_element_type=jnp.float32)
        for head in range(heads):
            grad_q = grad_qt[:, head * 128:(head + 1) * 128].T * SCALE
            dq_ref[:, cols[head]] = rotate_back(grad_q, cos_tab, sin_tab).astype(jnp.bfloat16)
        dko_ref[:, kcols] = grad_k[:rows]
        dkp_ref[:, kcols] = grad_k[rows:]
        dvo_ref[:, kcols] = grad_v[:rows]
        dvp_ref[:, kcols] = grad_v[rows:]


def attn_bwd(q_rot, kv_own, kv_prt, gout, attn, cos_tab, sin_tab, qpos, kpos, n_seq):
    tokens, q_cols = q_rot.shape
    kv_cols = kv_own.shape[1] // 2
    heads = q_cols // kv_cols
    groups = 2
    kv_blocks = kv_cols // HEAD_DIM // groups
    q_spec, k_spec, v_spec, tab, qpos_spec, kpos_spec = attn_specs(heads, groups, kv_blocks)
    kv_f32 = jax.ShapeDtypeStruct((tokens, kv_cols), jnp.float32)
    return pl.pallas_call(
        functools.partial(attn_bwd_kernel, heads),
        grid=(n_seq, kv_blocks),
        in_specs=[q_spec, k_spec, v_spec, k_spec, v_spec, q_spec, q_spec, tab, tab, qpos_spec, kpos_spec],
        out_specs=[q_spec, k_spec, k_spec, k_spec, k_spec],
        out_shape=[jax.ShapeDtypeStruct((tokens, q_cols), jnp.bfloat16), kv_f32, kv_f32, kv_f32, kv_f32],
        cost_estimate=pl.CostEstimate(flops=60 * 10 ** 9, bytes_accessed=tokens * q_cols * 12, transcendentals=tokens * q_cols * 2),
        compiler_params=pltpu.CompilerParams(dimension_semantics=("arbitrary", "arbitrary")),
        name="attn_bwd",
    )(q_rot, kv_own, kv_own, kv_prt, kv_prt, gout, attn, cos_tab, sin_tab, qpos, kpos)


def dw_kernel(own_idx, prt_idx, a0_ref, a1_ref, b0_ref, b1_ref, out_ref):
    out_ref[0] = jnp.dot(a0_ref[...], b0_ref[...], preferred_element_type=jnp.float32) + jnp.dot(a1_ref[...], b1_ref[...], preferred_element_type=jnp.float32)


def dw_blocks(own_idx, prt_idx, lhs_own, lhs_prt, rhs_own, rhs_prt, col0, ncols, tile):
    tokens = lhs_own.shape[1]
    nblk = own_idx.shape[0]
    first = col0 // tile
    grid_spec = pltpu.PrefetchScalarGridSpec(
        num_scalar_prefetch=2,
        grid=(ncols // tile, nblk),
        in_specs=[
            pl.BlockSpec((BLK, tokens), lambda j, i, oi, pi: (oi[i], 0)),
            pl.BlockSpec((BLK, tokens), lambda j, i, oi, pi: (pi[i], 0)),
            pl.BlockSpec((tokens, tile), lambda j, i, oi, pi: (0, first + j)),
            pl.BlockSpec((tokens, tile), lambda j, i, oi, pi: (0, first + j)),
        ],
        out_specs=pl.BlockSpec((1, BLK, tile), lambda j, i, oi, pi: (i, 0, j)),
    )
    return pl.pallas_call(
        dw_kernel,
        grid_spec=grid_spec,
        out_shape=jax.ShapeDtypeStruct((nblk, BLK, ncols), jnp.float32),
        cost_estimate=pl.CostEstimate(flops=4 * nblk * BLK * tokens * ncols, bytes_accessed=nblk * BLK * ncols * 4 + 4 * tokens * ncols + 4 * nblk * BLK * tokens, transcendentals=0),
        compiler_params=pltpu.CompilerParams(dimension_semantics=("arbitrary", "arbitrary")),
        name="dw",
    )(own_idx, prt_idx, lhs_own, lhs_prt, rhs_own, rhs_prt)


WO_PIECES = (('xyz', 0, 1280, 1280), ('yxz', 1280, 1280, 1280), ('zxy', 2560, 1536, 512))
WQ_PIECES = (('xyz', 0, 1024, 1024), ('yxz', 1024, 1024, 1024), ('xyz', 2048, 1024, 1024), ('yxz', 3072, 1024, 1024))
WKV_PIECES = (('zxy', 0, 1024, 1024), ('zyx', 1024, 512, 512), ('yxz', 1536, 512, 512))
BITS = {'y': 8, 'x': 4, 'z': 1}


def solution(mesh):
    fsdp_size, cp_size = mesh.shape['fsdp'], mesh.shape['cp']

    def swap(val, axis):
        if axis == 'z':
            return lax.ppermute(val, 'cp', [(i, i ^ 1) for i in range(cp_size)])
        bit = {'core': 1, 'x': 2, 'y': 4}[axis]
        return lax.ppermute(val, 'fsdp', [(i, i ^ bit) for i in range(fsdp_size)])

    def collect_full(local_part):
        return lax.all_gather(local_part, ALL_AXES, axis=0, tiled=True)

    def block_ids(order, first):
        own16 = lax.axis_index('fsdp') * 2 + lax.axis_index('cp')
        own_ids, prt_ids = [], []
        for second in (0, 1):
            for third in (0, 1):
                flip = BITS[order[0]] * first + BITS[order[1]] * second + BITS[order[2]] * third
                blk = own16 ^ flip
                own_ids.append(blk)
                prt_ids.append((blk // 4) * 2 + blk % 2)
        return jnp.stack(own_ids).astype(jnp.int32), jnp.stack(prt_ids).astype(jnp.int32)

    def core_half(mat_t):
        core = lax.axis_index('fsdp') % 2
        feats, tokens = mat_t.shape
        other = lax.dynamic_index_in_dim(mat_t.reshape(feats // (4 * BLK), 2, 2 * BLK, tokens), 1 - core, axis=1, keepdims=False)
        return swap(other.reshape(feats // 2, tokens), 'core')

    def tie(val, *others):
        return lax.optimization_barrier((val,) + others)[0]

    def send_first(operands, piece):
        order, col0, ncols, tile = piece
        send1 = dw_blocks(*block_ids(order, 1), *operands, col0, ncols, tile)
        return send1, swap(send1, order[0])

    def keep_first(operands, piece):
        order, col0, ncols, tile = piece
        return dw_blocks(*block_ids(order, 0), *operands, col0, ncols, tile)

    def send_second(piece, keep1, recv1):
        send2 = keep1[2:4] + recv1[2:4]
        return send2, swap(send2, piece[0][1])

    def send_third(piece, keep1, recv1, recv2):
        return swap(keep1[1] + recv1[1] + recv2[1], piece[0][2])

    def gain_sum(part):
        core = lax.axis_index('fsdp') % 2
        x_idx = lax.axis_index('fsdp') // 2 % 2
        y_idx = lax.axis_index('fsdp') // 4
        z_idx = lax.axis_index('cp')
        cur = part
        for axis, idx in (('y', y_idx), ('x', x_idx), ('core', core), ('z', z_idx)):
            halves = cur.reshape(2, -1, 128)
            cur = lax.dynamic_index_in_dim(halves, idx, 0, False) + swap(lax.dynamic_index_in_dim(halves, 1 - idx, 0, False), axis)
        return cur.reshape(-1)

    def block_step(hidden, tok_pos, grad_out, norm_gain, w_query, w_key, w_value, w_out):
        n_seq, n_rows, dim = hidden.shape
        tokens = n_seq * n_rows
        kv_cols = w_key.shape[1]
        wkv_full = collect_full(jnp.concatenate([w_key, w_value], axis=1))
        gain_full = collect_full(norm_gain).reshape(1, dim)
        wq_full = collect_full(w_query)
        wo_full = collect_full(w_out)

        x_bf = hidden.reshape(tokens, dim)
        dy = grad_out.reshape(tokens, dim)
        dy_prt = swap(dy, 'core')
        normed, normed_t = prep(x_bf, gain_full)
        normed_tp = core_half(normed_t)

        half = HEAD_DIM // 2
        inv_freq = ROPE_THETA ** (-jnp.arange(half, dtype=jnp.float32) / half)
        angles = tok_pos.reshape(tokens, 1).astype(jnp.float32) * inv_freq
        cos_tab = jnp.concatenate([jnp.cos(angles)] * 2, axis=1)
        sin_tab = jnp.concatenate([-jnp.sin(angles), jnp.sin(angles)], axis=1)
        prt_pos = swap(tok_pos, 'z')
        qpos = tok_pos.reshape(n_seq, 1, n_rows)
        kpos = jnp.concatenate([tok_pos, prt_pos], axis=1).reshape(n_seq, 2 * n_rows, 1)

        kv_lin = jnp.dot(normed, wkv_full, preferred_element_type=jnp.float32)
        kv_own = rope_kv(kv_lin, cos_tab, sin_tab)
        kv_prt = swap(kv_own, 'z')
        q_lin = jnp.dot(normed, wq_full, preferred_element_type=jnp.float32)
        attn, attn_t, q_rot = attn_fwd(q_lin, kv_own, kv_prt, cos_tab, sin_tab, qpos, kpos, n_seq)
        attn_tp = core_half(attn_t)

        wo_ops = (attn_t, attn_tp, dy, dy_prt)
        wo_sent = [send_first(wo_ops, piece) for piece in WO_PIECES]
        wo_late = (attn_t, attn_tp, dy, tie(dy_prt, *[sent for sent, _ in wo_sent]))
        wo_keep = [keep_first(wo_late, piece) for piece in WO_PIECES]

        gout = lax.dot_general(tie(dy, *wo_keep), wo_full, NT, preferred_element_type=jnp.float32).astype(jnp.bfloat16)
        dq, dk_own, dv_own, dk_prt, dv_prt = attn_bwd(q_rot, kv_own, kv_prt, gout, attn, cos_tab, sin_tab, qpos, kpos, n_seq)
        dq_prt = swap(dq, 'core')
        dk_recv = swap(dk_prt, 'z')
        dv_recv = swap(dv_prt, 'z')

        wo_keep = [tie(keep, dq) for keep in wo_keep]
        wo_sent2 = [send_second(piece, keep, recv) for piece, keep, (_, recv) in zip(WO_PIECES, wo_keep, wo_sent)]
        wq_ops = (normed_t, normed_tp, dq, tie(dq_prt, *[sent for sent, _ in wo_sent2]))
        wq_sent = [send_first(wq_ops, piece) for piece in WQ_PIECES]
        wq_late = (normed_t, normed_tp, dq, tie(dq_prt, *[sent for sent, _ in wq_sent]))
        wq_keep = [keep_first(wq_late, piece) for piece in WQ_PIECES]

        result = (x_bf.astype(jnp.float32) + jnp.dot(tie(attn, *wq_keep), wo_full, preferred_element_type=jnp.float32)).astype(jnp.bfloat16)
        grad_nq = lax.dot_general(tie(dq, result), wq_full, NT, preferred_element_type=jnp.float32)

        dk_own, dv_own = lax.optimization_barrier((dk_own, dv_own, grad_nq))[:2]
        dkv = finish_dkv(dk_own, dk_recv, dv_own, dv_recv, cos_tab, sin_tab)
        dkv_prt = swap(dkv, 'core')
        wkv_ops = (normed_t, normed_tp, dkv, dkv_prt)
        wkv_sent = [send_first(wkv_ops, piece) for piece in WKV_PIECES]
        wkv_late = (normed_t, normed_tp, dkv, tie(dkv_prt, *[sent for sent, _ in wkv_sent]))
        wkv_keep = [keep_first(wkv_late, piece) for piece in WKV_PIECES]

        def finish(pieces, keeps, sent, sent2):
            if sent2 is None:
                sent2 = [send_second(piece, keep, recv) for piece, keep, (_, recv) in zip(pieces, keeps, sent)]
            outs = []
            for piece, keep, (_, recv1), (_, recv2) in zip(pieces, keeps, sent, sent2):
                recv3 = send_third(piece, keep, recv1, recv2)
                outs.append(keep[0] + recv1[0] + recv2[0] + recv3)
            return jnp.concatenate(outs, axis=1)

        grad_wo = finish(WO_PIECES, wo_keep, wo_sent, wo_sent2)
        grad_wq = finish(WQ_PIECES, wq_keep, wq_sent, None)
        grad_wkv = finish(WKV_PIECES, wkv_keep, wkv_sent, None)

        grad_normed = grad_nq + lax.dot_general(tie(dkv, *wkv_keep), wkv_full, NT, preferred_element_type=jnp.float32)
        grad_hidden, gain_part = epilogue(grad_normed, x_bf, dy, gain_full)
        return (result.reshape(hidden.shape), grad_hidden.reshape(hidden.shape), grad_wq, grad_wkv[:, :kv_cols], grad_wkv[:, kv_cols:], grad_wo, gain_sum(gain_part))

    row_spec = P('fsdp', 'cp', None)
    pos_spec = P('fsdp', 'cp')
    weight_spec = P(ALL_AXES, None)
    gain_spec = P(ALL_AXES)
    return jax.shard_map(block_step, mesh=mesh, in_specs=(row_spec, pos_spec, row_spec, gain_spec, weight_spec, weight_spec, weight_spec, weight_spec), out_specs=(row_spec, row_spec, weight_spec, weight_spec, weight_spec, weight_spec, gain_spec), check_vma=False)
```

```python
import functools

import jax
import jax.numpy as jnp
from jax import lax
from jax.experimental import pallas as pl
from jax.experimental.pallas import tpu as pltpu
from jax.sharding import PartitionSpec as P


HEAD_DIM = 128
ROPE_THETA = 1000000.0
RMS_EPS = 1e-5
NEG_BIG = -1e30
SCALE = HEAD_DIM ** -0.5
ALL_AXES = ('fsdp', 'cp')
NT = (((1,), (1,)), ((), ()))
TN = (((0,), (0,)), ((), ()))
BLK = 256


def rotate(val, cos_tab, sin_tab):
    return val * cos_tab + pltpu.roll(val, 64, 1) * sin_tab


def rotate_back(val, cos_tab, sin_tab):
    return val * cos_tab - pltpu.roll(val, 64, 1) * sin_tab


def rope_kv_kernel(kv_ref, cos_ref, sin_ref, out_ref):
    cos_tab, sin_tab = cos_ref[...], sin_ref[...]
    width = kv_ref.shape[1]
    for col in range(0, width // 2, HEAD_DIM):
        out_ref[:, col:col + HEAD_DIM] = rotate(kv_ref[:, col:col + HEAD_DIM], cos_tab, sin_tab).astype(jnp.bfloat16)
    out_ref[:, width // 2:] = kv_ref[:, width // 2:].astype(jnp.bfloat16)


def rope_kv(kv_lin, cos_tab, sin_tab):
    tokens, width = kv_lin.shape
    rows = 128
    return pl.pallas_call(
        rope_kv_kernel,
        grid=(tokens // rows,),
        in_specs=[pl.BlockSpec((rows, width), lambda i: (i, 0)), pl.BlockSpec((rows, HEAD_DIM), lambda i: (i, 0)), pl.BlockSpec((rows, HEAD_DIM), lambda i: (i, 0))],
        out_specs=pl.BlockSpec((rows, width), lambda i: (i, 0)),
        out_shape=jax.ShapeDtypeStruct((tokens, width), jnp.bfloat16),
        cost_estimate=pl.CostEstimate(flops=tokens * width * 1000, bytes_accessed=tokens * width * 6, transcendentals=0),
        name="rope_kv",
    )(kv_lin, cos_tab, sin_tab)


def finish_dkv_kernel(dk_ref, dkr_ref, dv_ref, dvr_ref, cos_ref, sin_ref, out_ref):
    cos_tab, sin_tab = cos_ref[...], sin_ref[...]
    width = dk_ref.shape[1]
    for col in range(0, width, HEAD_DIM):
        cols = slice(col, col + HEAD_DIM)
        out_ref[:, cols] = rotate_back((dk_ref[:, cols] + dkr_ref[:, cols]) * SCALE, cos_tab, sin_tab).astype(jnp.bfloat16)
    out_ref[:, width:] = (dv_ref[...] + dvr_ref[...]).astype(jnp.bfloat16)


def finish_dkv(dk_own, dk_recv, dv_own, dv_recv, cos_tab, sin_tab):
    tokens, width = dk_own.shape
    rows = 128
    part = pl.BlockSpec((rows, width), lambda i: (i, 0))
    tab = pl.BlockSpec((rows, HEAD_DIM), lambda i: (i, 0))
    return pl.pallas_call(
        finish_dkv_kernel,
        grid=(tokens // rows,),
        in_specs=[part, part, part, part, tab, tab],
        out_specs=pl.BlockSpec((rows, 2 * width), lambda i: (i, 0)),
        out_shape=jax.ShapeDtypeStruct((tokens, 2 * width), jnp.bfloat16),
        cost_estimate=pl.CostEstimate(flops=tokens * width * 2000, bytes_accessed=tokens * width * 20, transcendentals=0),
        name="finish_dkv",
    )(dk_own, dk_recv, dv_own, dv_recv, cos_tab, sin_tab)


def prep_kernel(x_ref, gain_ref, out_ref, out_t_ref):
    x_f32 = x_ref[...].astype(jnp.float32)
    inv_rms = lax.rsqrt(jnp.mean(x_f32 * x_f32, axis=-1, keepdims=True) + RMS_EPS)
    for col in range(0, x_ref.shape[1], 128):
        cols = slice(col, col + 128)
        normed = (x_ref[:, cols].astype(jnp.float32) * inv_rms * gain_ref[:, cols]).astype(jnp.bfloat16)
        out_ref[:, cols] = normed
        out_t_ref[cols, :] = normed.astype(jnp.float32).T.astype(jnp.bfloat16)


def prep(x_bf, gain):
    tokens, dim = x_bf.shape
    rows = 128
    return pl.pallas_call(
        prep_kernel,
        grid=(tokens // rows,),
        in_specs=[pl.BlockSpec((rows, dim), lambda i: (i, 0)), pl.BlockSpec((1, dim), lambda i: (0, 0))],
        out_specs=[pl.BlockSpec((rows, dim), lambda i: (i, 0)), pl.BlockSpec((dim, rows), lambda i: (0, i))],
        out_shape=[jax.ShapeDtypeStruct((tokens, dim), jnp.bfloat16), jax.ShapeDtypeStruct((dim, tokens), jnp.bfloat16)],
        cost_estimate=pl.CostEstimate(flops=tokens * dim * 1000, bytes_accessed=tokens * dim * 6, transcendentals=0),
        name="prep",
    )(x_bf, gain)


def epilogue_kernel(dr_ref, x_ref, dy_ref, gain_ref, out_ref, gain_out_ref):
    x_f32 = x_ref[...].astype(jnp.float32)
    inv_rms = lax.rsqrt(jnp.mean(x_f32 * x_f32, axis=-1, keepdims=True) + RMS_EPS)
    x_hat = x_f32 * inv_rms
    grad_normed = dr_ref[...]
    gain_part = jnp.sum(grad_normed * x_hat, axis=0, keepdims=True)

    @pl.when(pl.program_id(0) == 0)
    def _():
        gain_out_ref[...] = gain_part

    @pl.when(pl.program_id(0) > 0)
    def _():
        gain_out_ref[...] += gain_part

    grad_xhat = grad_normed * gain_ref[...]
    grad_x = inv_rms * (grad_xhat - x_hat * jnp.mean(grad_xhat * x_hat, axis=-1, keepdims=True))
    out_ref[...] = (dy_ref[...].astype(jnp.float32) + grad_x).astype(jnp.bfloat16)


def epilogue(grad_normed, x_bf, dy, gain):
    tokens, dim = x_bf.shape
    rows = 64
    full = pl.BlockSpec((rows, dim), lambda i: (i, 0))
    vec = pl.BlockSpec((1, dim), lambda i: (0, 0))
    return pl.pallas_call(
        epilogue_kernel,
        grid=(tokens // rows,),
        in_specs=[full, full, full, vec],
        out_specs=[full, vec],
        out_shape=[jax.ShapeDtypeStruct((tokens, dim), jnp.bfloat16), jax.ShapeDtypeStruct((1, dim), jnp.float32)],
        cost_estimate=pl.CostEstimate(flops=tokens * dim * 1000, bytes_accessed=tokens * dim * 10, transcendentals=0),
        name="epilogue",
    )(grad_normed, x_bf, dy, gain)


def scores_t(keys, queries, mask_t, heads):
    st = lax.dot_general(keys, queries, NT, preferred_element_type=jnp.float32) * SCALE
    return jnp.where(jnp.concatenate([mask_t] * heads, axis=1), st, NEG_BIG)


def attn_fwd_kernel(heads, q_ref, ko_ref, vo_ref, kp_ref, vp_ref, cos_ref, sin_ref, qpos_ref, kpos_ref, o_ref, ot_ref, qr_ref):
    cos_tab, sin_tab = cos_ref[...], sin_ref[...]
    mask_t = kpos_ref[0] <= qpos_ref[0]
    groups = ko_ref.shape[1] // HEAD_DIM
    for grp in range(groups):
        kcols = slice(grp * HEAD_DIM, (grp + 1) * HEAD_DIM)
        keys = jnp.concatenate([ko_ref[:, kcols], kp_ref[:, kcols]], axis=0)
        vals = jnp.concatenate([vo_ref[:, kcols], vp_ref[:, kcols]], axis=0)
        rot = []
        for head in range(heads):
            col = (grp * heads + head) * HEAD_DIM
            q_rot = rotate(q_ref[:, col:col + HEAD_DIM], cos_tab, sin_tab).astype(jnp.bfloat16)
            qr_ref[:, col:col + HEAD_DIM] = q_rot
            rot.append(q_rot)
        queries = jnp.concatenate(rot, axis=0)
        st = scores_t(keys, queries, mask_t, heads)
        row_max = jnp.max(st, axis=0, keepdims=True)
        probs = jnp.exp(st - row_max)
        row_sum = jnp.sum(probs, axis=0, keepdims=True)
        out_t = lax.dot_general(vals, probs.astype(jnp.bfloat16), TN, preferred_element_type=jnp.float32) / row_sum
        for head in range(heads):
            col = (grp * heads + head) * HEAD_DIM
            part = out_t[:, head * 128:(head + 1) * 128]
            ot_ref[col:col + HEAD_DIM, :] = part.astype(jnp.bfloat16)
            o_ref[:, col:col + HEAD_DIM] = part.T.astype(jnp.bfloat16)


def attn_specs(heads, groups, kv_blocks, first=0):
    rows = 128
    q_spec = pl.BlockSpec((rows, groups * heads * HEAD_DIM), lambda b, g: (b, first + g))
    k_spec = pl.BlockSpec((rows, groups * HEAD_DIM), lambda b, g: (b, first + g))
    v_spec = pl.BlockSpec((rows, groups * HEAD_DIM), lambda b, g: (b, kv_blocks + first + g))
    tab = pl.BlockSpec((rows, HEAD_DIM), lambda b, g: (b, 0))
    qpos = pl.BlockSpec((1, 1, rows), lambda b, g: (b, 0, 0))
    kpos = pl.BlockSpec((1, 2 * rows, 1), lambda b, g: (b, 0, 0))
    return q_spec, k_spec, v_spec, tab, qpos, kpos


def attn_fwd_half(heads, q_ref, ko_ref, vo_ref, kp_ref, vp_ref, cos_ref, sin_ref, qpos_ref, kpos_ref, *rest):
    attn_fwd_kernel(heads, q_ref, ko_ref, vo_ref, kp_ref, vp_ref, cos_ref, sin_ref, qpos_ref, kpos_ref, *rest[-3:])


def attn_fwd(part, parts, q_part, kv_own, kv_prt, cos_tab, sin_tab, qpos, kpos, n_seq, prev):
    tokens, part_cols = q_part.shape
    q_cols = part_cols * parts
    kv_cols = kv_own.shape[1] // 2
    heads = q_cols // kv_cols
    groups = 2
    kv_blocks = kv_cols // HEAD_DIM // groups
    blocks = kv_blocks // parts
    first = part * blocks
    q_spec, k_spec, v_spec, tab, qpos_spec, kpos_spec = attn_specs(heads, groups, kv_blocks, first)
    rows = tokens // n_seq
    in_spec = pl.BlockSpec((rows, groups * heads * HEAD_DIM), lambda b, g: (b, g))
    return pl.pallas_call(
        functools.partial(attn_fwd_half, heads),
        grid=(n_seq, blocks),
        in_specs=[in_spec, k_spec, v_spec, k_spec, v_spec, tab, tab, qpos_spec, kpos_spec] + [pl.BlockSpec(memory_space=pl.ANY)] * len(prev),
        out_specs=[q_spec, pl.BlockSpec((groups * heads * HEAD_DIM, rows), lambda b, g: (first + g, b)), q_spec],
        out_shape=[jax.ShapeDtypeStruct((tokens, q_cols), jnp.bfloat16), jax.ShapeDtypeStruct((q_cols, tokens), jnp.bfloat16), jax.ShapeDtypeStruct((tokens, q_cols), jnp.bfloat16)],
        input_output_aliases={9 + i: i for i in range(len(prev))},
        cost_estimate=pl.CostEstimate(flops=15 * 10 ** 9, bytes_accessed=tokens * part_cols * 10, transcendentals=tokens * part_cols * 2),
        compiler_params=pltpu.CompilerParams(dimension_semantics=("arbitrary", "arbitrary")),
        name="attn_fwd",
    )(q_part, kv_own, kv_own, kv_prt, kv_prt, cos_tab, sin_tab, qpos, kpos, *prev)


def attn_bwd_kernel(heads, q_ref, ko_ref, vo_ref, kp_ref, vp_ref, do_ref, o_ref, cos_ref, sin_ref, qpos_ref, kpos_ref, dq_ref, dko_ref, dvo_ref, dkp_ref, dvp_ref):
    cos_tab, sin_tab = cos_ref[...], sin_ref[...]
    mask_t = kpos_ref[0] <= qpos_ref[0]
    groups = ko_ref.shape[1] // HEAD_DIM
    rows = q_ref.shape[0]
    for grp in range(groups):
        kcols = slice(grp * HEAD_DIM, (grp + 1) * HEAD_DIM)
        keys = jnp.concatenate([ko_ref[:, kcols], kp_ref[:, kcols]], axis=0)
        vals = jnp.concatenate([vo_ref[:, kcols], vp_ref[:, kcols]], axis=0)
        cols = [slice((grp * heads + head) * HEAD_DIM, (grp * heads + head + 1) * HEAD_DIM) for head in range(heads)]
        queries = jnp.concatenate([q_ref[:, c] for c in cols], axis=0)
        gout = jnp.concatenate([do_ref[:, c] for c in cols], axis=0)
        delta = jnp.concatenate([jnp.sum((do_ref[:, c].astype(jnp.float32) * o_ref[:, c].astype(jnp.float32)).T, axis=0, keepdims=True) for c in cols], axis=1)
        st = scores_t(keys, queries, mask_t, heads)
        row_max = jnp.max(st, axis=0, keepdims=True)
        probs = jnp.exp(st - row_max)
        probs = probs * (1.0 / jnp.sum(probs, axis=0, keepdims=True))
        grad_p = lax.dot_general(vals, gout, NT, preferred_element_type=jnp.float32)
        grad_s = (probs * (grad_p - delta)).astype(jnp.bfloat16)
        grad_v = jnp.dot(probs.astype(jnp.bfloat16), gout, preferred_element_type=jnp.float32)
        grad_k = jnp.dot(grad_s, queries, preferred_element_type=jnp.float32)
        grad_qt = lax.dot_general(keys, grad_s, TN, preferred_element_type=jnp.float32)
        for head in range(heads):
            grad_q = grad_qt[:, head * 128:(head + 1) * 128].T * SCALE
            dq_ref[:, cols[head]] = rotate_back(grad_q, cos_tab, sin_tab).astype(jnp.bfloat16)
        dko_ref[:, kcols] = grad_k[:rows]
        dkp_ref[:, kcols] = grad_k[rows:]
        dvo_ref[:, kcols] = grad_v[:rows]
        dvp_ref[:, kcols] = grad_v[rows:]


def attn_bwd(q_rot, kv_own, kv_prt, gout, attn, cos_tab, sin_tab, qpos, kpos, n_seq):
    tokens, q_cols = q_rot.shape
    kv_cols = kv_own.shape[1] // 2
    heads = q_cols // kv_cols
    groups = 2
    kv_blocks = kv_cols // HEAD_DIM // groups
    q_spec, k_spec, v_spec, tab, qpos_spec, kpos_spec = attn_specs(heads, groups, kv_blocks)
    kv_f32 = jax.ShapeDtypeStruct((tokens, kv_cols), jnp.float32)
    return pl.pallas_call(
        functools.partial(attn_bwd_kernel, heads),
        grid=(n_seq, kv_blocks),
        in_specs=[q_spec, k_spec, v_spec, k_spec, v_spec, q_spec, q_spec, tab, tab, qpos_spec, kpos_spec],
        out_specs=[q_spec, k_spec, k_spec, k_spec, k_spec],
        out_shape=[jax.ShapeDtypeStruct((tokens, q_cols), jnp.bfloat16), kv_f32, kv_f32, kv_f32, kv_f32],
        cost_estimate=pl.CostEstimate(flops=60 * 10 ** 9, bytes_accessed=tokens * q_cols * 12, transcendentals=tokens * q_cols * 2),
        compiler_params=pltpu.CompilerParams(dimension_semantics=("arbitrary", "arbitrary")),
        name="attn_bwd",
    )(q_rot, kv_own, kv_own, kv_prt, kv_prt, gout, attn, cos_tab, sin_tab, qpos, kpos)


def dw_kernel(own_idx, prt_idx, lhs_own_ref, lhs_prt_ref, b0_ref, b1_ref, out_ref, lhs_buf, sem):
    nblk = out_ref.shape[0]
    tokens = b0_ref.shape[0]

    @pl.when(pl.program_id(0) == 0)
    def _():
        copies = []
        for i in range(nblk):
            rows = pl.ds(i * BLK, BLK)
            for idx, src, col in ((own_idx, lhs_own_ref, 0), (prt_idx, lhs_prt_ref, tokens)):
                start = pl.multiple_of(idx[i] * BLK, BLK)
                copies.append(pltpu.make_async_copy(src.at[pl.ds(start, BLK), :], lhs_buf.at[rows, pl.ds(col, tokens)], sem))
        for copy in copies:
            copy.start()
        for copy in copies:
            copy.wait()

    acc = jnp.dot(lhs_buf[:, :tokens], b0_ref[...], preferred_element_type=jnp.float32)
    acc += jnp.dot(lhs_buf[:, tokens:], b1_ref[...], preferred_element_type=jnp.float32)
    out_ref[...] = acc.reshape(out_ref.shape)


def dw_blocks(own_idx, prt_idx, lhs_own, lhs_prt, rhs_own, rhs_prt, col0, ncols):
    tokens = lhs_own.shape[1]
    nblk = own_idx.shape[0]
    tile = 256
    first = col0 // tile
    any_spec = pl.BlockSpec(memory_space=pl.ANY)
    rhs_spec = pl.BlockSpec((tokens, tile), lambda j, oi, pi: (0, first + j))
    grid_spec = pltpu.PrefetchScalarGridSpec(
        num_scalar_prefetch=2,
        grid=(ncols // tile,),
        in_specs=[any_spec, any_spec, rhs_spec, rhs_spec],
        out_specs=pl.BlockSpec((nblk, BLK, tile), lambda j, oi, pi: (0, 0, j)),
        scratch_shapes=[pltpu.VMEM((nblk * BLK, 2 * tokens), jnp.bfloat16), pltpu.SemaphoreType.DMA],
    )
    return pl.pallas_call(
        dw_kernel,
        grid_spec=grid_spec,
        out_shape=jax.ShapeDtypeStruct((nblk, BLK, ncols), jnp.float32),
        cost_estimate=pl.CostEstimate(flops=4 * nblk * BLK * tokens * ncols, bytes_accessed=nblk * BLK * ncols * 4 + 4 * tokens * ncols + 4 * nblk * BLK * tokens, transcendentals=0),
        compiler_params=pltpu.CompilerParams(dimension_semantics=("arbitrary",)),
        name="dw",
    )(own_idx, prt_idx, lhs_own, lhs_prt, rhs_own, rhs_prt)


WO_PIECES = (('xyz', 0, 1280), ('yxz', 1280, 1280), ('zxy', 2560, 1536))
WQ_PIECES = (('xyz', 0, 1024), ('yxz', 2048, 1024), ('xyz', 1024, 1024), ('yxz', 3072, 1024))
WKV_PIECES = (('zxy', 0, 1024), ('yxz', 1024, 1024))
BITS = {'y': 8, 'x': 4, 'z': 1}


def solution(mesh):
    fsdp_size, cp_size = mesh.shape['fsdp'], mesh.shape['cp']

    def swap(val, axis):
        if axis == 'z':
            return lax.ppermute(val, 'cp', [(i, i ^ 1) for i in range(cp_size)])
        bit = {'core': 1, 'x': 2, 'y': 4}[axis]
        return lax.ppermute(val, 'fsdp', [(i, i ^ bit) for i in range(fsdp_size)])

    def collect_full(local_part):
        return lax.all_gather(local_part, ALL_AXES, axis=0, tiled=True)

    def block_ids(order, first):
        own16 = lax.axis_index('fsdp') * 2 + lax.axis_index('cp')
        own_ids, prt_ids = [], []
        for second in (0, 1):
            for third in (0, 1):
                flip = BITS[order[0]] * first + BITS[order[1]] * second + BITS[order[2]] * third
                blk = own16 ^ flip
                own_ids.append(blk)
                prt_ids.append((blk // 4) * 2 + blk % 2)
        return jnp.stack(own_ids).astype(jnp.int32), jnp.stack(prt_ids).astype(jnp.int32)

    def core_half(mat_t):
        core = lax.axis_index('fsdp') % 2
        feats, tokens = mat_t.shape
        other = lax.dynamic_index_in_dim(mat_t.reshape(feats // (4 * BLK), 2, 2 * BLK, tokens), 1 - core, axis=1, keepdims=False)
        return swap(other.reshape(feats // 2, tokens), 'core')

    def tie(val, *others):
        return lax.optimization_barrier((val,) + others)[0]

    def send_first(operands, piece):
        order, col0, ncols = piece
        send1 = dw_blocks(*block_ids(order, 1), *operands, col0, ncols)
        return send1, swap(send1, order[0])

    def keep_first(operands, order, col0, ncols):
        return dw_blocks(*block_ids(order, 0), *operands, col0, ncols)

    def send_second(piece, keep1, recv1):
        send2 = keep1[2:4] + recv1[2:4]
        return send2, swap(send2, piece[0][1])

    def send_third(piece, keep1, recv1, recv2):
        return swap(keep1[1] + recv1[1] + recv2[1], piece[0][2])

    def finish(pieces, keeps, sent, sent2):
        recv3 = [send_third(piece, keep, recv1, recv2) for piece, keep, (_, recv1), (_, recv2) in zip(pieces, keeps, sent, sent2)]
        return [keep[0] + recv1[0] + recv2[0] + last for keep, (_, recv1), (_, recv2), last in zip(keeps, sent, sent2, recv3)]

    def gain_sum(part):
        fsdp = lax.axis_index('fsdp')
        cur = part.reshape(2, 2, 2, 2, 2, 128)
        for axis, dim, idx in (('core', 2, fsdp % 2), ('z', 2, lax.axis_index('cp')), ('y', 0, fsdp // 4), ('x', 0, fsdp // 2 % 2)):
            moved = swap(lax.dynamic_index_in_dim(cur, 1 - idx, dim, False), axis)
            cur = lax.dynamic_index_in_dim(cur, idx, dim, False) + moved
        return cur.reshape(-1)

    def block_step(hidden, tok_pos, grad_out, norm_gain, w_query, w_key, w_value, w_out):
        n_seq, n_rows, dim = hidden.shape
        tokens = n_seq * n_rows
        q_cols = w_query.shape[1]
        half_cols = q_cols // 2
        wkv_full = collect_full(jnp.concatenate([w_key, w_value], axis=1))
        gain_full = collect_full(norm_gain).reshape(1, dim)
        wq_other = swap(w_query, 'z')

        x_bf = hidden.reshape(tokens, dim)
        dy = grad_out.reshape(tokens, dim)
        dy_prt = swap(dy, 'core')
        normed, normed_t = prep(x_bf, gain_full)
        normed_tp = core_half(normed_t)
        wq_other = tie(wq_other, normed)
        z_low = lax.axis_index('cp') == 0
        wq_pair = jnp.concatenate([jnp.where(z_low, w_query, wq_other), jnp.where(z_low, wq_other, w_query)], axis=0)
        wq_half = [lax.all_gather(wq_pair[:, i * half_cols:(i + 1) * half_cols], 'fsdp', axis=0, tiled=True) for i in range(2)]
        wo_full = collect_full(w_out)

        half = HEAD_DIM // 2
        inv_freq = ROPE_THETA ** (-jnp.arange(half, dtype=jnp.float32) / half)
        angles = tok_pos.reshape(tokens, 1).astype(jnp.float32) * inv_freq
        cos_tab = jnp.concatenate([jnp.cos(angles)] * 2, axis=1)
        sin_tab = jnp.concatenate([-jnp.sin(angles), jnp.sin(angles)], axis=1)
        prt_pos = swap(tok_pos, 'z')
        qpos = tok_pos.reshape(n_seq, 1, n_rows)
        kpos = jnp.concatenate([tok_pos, prt_pos], axis=1).reshape(n_seq, 2 * n_rows, 1)

        kv_lin = jnp.dot(normed, wkv_full, preferred_element_type=jnp.float32)
        kv_own = rope_kv(kv_lin, cos_tab, sin_tab)
        kv_prt = swap(kv_own, 'z')
        fwd_out = ()
        for i in range(2):
            q_part = jnp.dot(tie(normed, *fwd_out[:1]), wq_half[i], preferred_element_type=jnp.float32)
            fwd_out = attn_fwd(i, 2, q_part, kv_own, kv_prt, cos_tab, sin_tab, qpos, kpos, n_seq, fwd_out)
        attn, attn_t, q_rot = fwd_out
        attn_tp = core_half(attn_t)

        wo_ops = (attn_t, attn_tp, dy, dy_prt)
        wo_sent = [send_first(wo_ops, piece) for piece in WO_PIECES]
        wo_late = (attn_t, attn_tp, dy, tie(dy_prt, *[sent for sent, _ in wo_sent]))
        wo_keep = [keep_first(wo_late, *piece) for piece in WO_PIECES]

        gout = lax.dot_general(tie(dy, *wo_keep), wo_full, NT, preferred_element_type=jnp.float32).astype(jnp.bfloat16)
        dq, dk_own, dv_own, dk_prt, dv_prt = attn_bwd(q_rot, kv_own, kv_prt, gout, attn, cos_tab, sin_tab, qpos, kpos, n_seq)
        dq_prt = swap(dq, 'core')
        dk_recv = swap(dk_prt, 'z')
        dv_recv = swap(dv_prt, 'z')

        wo_keep = [tie(keep, dq) for keep in wo_keep]
        wo_sent2 = [send_second(piece, keep, recv) for piece, keep, (_, recv) in zip(WO_PIECES, wo_keep, wo_sent)]
        wq_ops = (normed_t, normed_tp, dq, tie(dq_prt, *[sent for sent, _ in wo_sent2]))
        wq_sent = [send_first(wq_ops, piece) for piece in WQ_PIECES]
        wq_late = (normed_t, normed_tp, dq, tie(dq_prt, *[sent for sent, _ in wq_sent]))
        wq_keep = [keep_first(wq_late, *piece) for piece in WQ_PIECES]

        result = (x_bf.astype(jnp.float32) + jnp.dot(tie(attn, *wq_keep), wo_full, preferred_element_type=jnp.float32)).astype(jnp.bfloat16)
        dq_late = tie(dq, result)
        grad_nq = lax.dot_general(dq_late[:, :half_cols], wq_half[0], NT, preferred_element_type=jnp.float32)
        grad_nq = grad_nq + lax.dot_general(dq_late[:, half_cols:], wq_half[1], NT, preferred_element_type=jnp.float32)

        dk_own, dv_own = lax.optimization_barrier((dk_own, dv_own, grad_nq))[:2]
        dkv = finish_dkv(dk_own, dk_recv, dv_own, dv_recv, cos_tab, sin_tab)
        dkv_prt = swap(dkv, 'core')
        wkv_ops = (normed_t, normed_tp, dkv, dkv_prt)
        wkv_sent = [send_first(wkv_ops, piece) for piece in WKV_PIECES]

        wq_sent2 = []
        for piece, keep, (_, recv) in zip(WQ_PIECES, wq_keep, wq_sent):
            keep = tie(keep, *[sent for sent, _ in wkv_sent])
            wq_sent2.append(send_second(piece, keep, recv))
        wkv_late = (normed_t, normed_tp, dkv, tie(dkv_prt, wq_sent2[0][0], wq_sent2[1][0]))
        wkv_keep = [keep_first(wkv_late, *piece) for piece in WKV_PIECES]
        grad_normed = grad_nq + lax.dot_general(tie(dkv, *wkv_keep), wkv_full, NT, preferred_element_type=jnp.float32)
        grad_hidden, gain_part = epilogue(grad_normed, x_bf, dy, gain_full)
        grad_gain = gain_sum(gain_part)

        wkv_sent2 = [send_second(piece, keep, recv) for piece, keep, (_, recv) in zip(WKV_PIECES, wkv_keep, wkv_sent)]
        grad_wo = jnp.concatenate(finish(WO_PIECES, wo_keep, wo_sent, wo_sent2), axis=1)
        wq_out = finish(WQ_PIECES, wq_keep, wq_sent, wq_sent2)
        grad_wq = jnp.concatenate([wq_out[0], wq_out[2], wq_out[1], wq_out[3]], axis=1)
        grad_wk, grad_wv = finish(WKV_PIECES, wkv_keep, wkv_sent, wkv_sent2)
        return (result.reshape(hidden.shape), grad_hidden.reshape(hidden.shape), grad_wq, grad_wk, grad_wv, grad_wo, grad_gain)

    row_spec = P('fsdp', 'cp', None)
    pos_spec = P('fsdp', 'cp')
    weight_spec = P(ALL_AXES, None)
    gain_spec = P(ALL_AXES)
    return jax.shard_map(block_step, mesh=mesh, in_specs=(row_spec, pos_spec, row_spec, gain_spec, weight_spec, weight_spec, weight_spec, weight_spec), out_specs=(row_spec, row_spec, weight_spec, weight_spec, weight_spec, weight_spec, gain_spec), check_vma=False)
```

```python
import functools

import jax
import jax.numpy as jnp
from jax import lax
from jax.experimental import pallas as pl
from jax.experimental.pallas import tpu as pltpu
from jax.sharding import PartitionSpec as P


HEAD_DIM = 128
ROPE_THETA = 1000000.0
RMS_EPS = 1e-5
NEG_BIG = -1e30
SCALE = HEAD_DIM ** -0.5
ALL_AXES = ('fsdp', 'cp')
NT = (((1,), (1,)), ((), ()))
TN = (((0,), (0,)), ((), ()))
BLK = 256

CHUNKS = (3, 2, 2, 1)
GROUP = 6 * HEAD_DIM


def rotate(val, cos_tab, sin_tab):
    return val * cos_tab + pltpu.roll(val, 64, 1) * sin_tab


def rotate_back(val, cos_tab, sin_tab):
    return val * cos_tab - pltpu.roll(val, 64, 1) * sin_tab


def prep_kernel(x_ref, gain_ref, out_ref, out_t_ref):
    x_f32 = x_ref[...].astype(jnp.float32)
    inv_rms = lax.rsqrt(jnp.mean(x_f32 * x_f32, axis=-1, keepdims=True) + RMS_EPS)
    for col in range(0, x_ref.shape[1], 128):
        cols = slice(col, col + 128)
        normed = (x_ref[:, cols].astype(jnp.float32) * inv_rms * gain_ref[:, cols]).astype(jnp.bfloat16)
        out_ref[:, cols] = normed
        out_t_ref[cols, :] = normed.astype(jnp.float32).T.astype(jnp.bfloat16)


def prep(x_bf, gain):
    tokens, dim = x_bf.shape
    rows = 128
    return pl.pallas_call(
        prep_kernel,
        grid=(tokens // rows,),
        in_specs=[pl.BlockSpec((rows, dim), lambda i: (i, 0)), pl.BlockSpec((1, dim), lambda i: (0, 0))],
        out_specs=[pl.BlockSpec((rows, dim), lambda i: (i, 0)), pl.BlockSpec((dim, rows), lambda i: (0, i))],
        out_shape=[jax.ShapeDtypeStruct((tokens, dim), jnp.bfloat16), jax.ShapeDtypeStruct((dim, tokens), jnp.bfloat16)],
        cost_estimate=pl.CostEstimate(flops=tokens * dim * 1000, bytes_accessed=tokens * dim * 6, transcendentals=0),
        name="prep",
    )(x_bf, gain)


def epilogue_kernel(dr_ref, x_ref, dy_ref, gain_ref, out_ref, gain_out_ref):
    x_f32 = x_ref[...].astype(jnp.float32)
    inv_rms = lax.rsqrt(jnp.mean(x_f32 * x_f32, axis=-1, keepdims=True) + RMS_EPS)
    x_hat = x_f32 * inv_rms
    grad_normed = dr_ref[...]
    gain_part = jnp.sum(grad_normed * x_hat, axis=0, keepdims=True)

    @pl.when(pl.program_id(0) == 0)
    def _():
        gain_out_ref[...] = gain_part

    @pl.when(pl.program_id(0) > 0)
    def _():
        gain_out_ref[...] += gain_part

    grad_xhat = grad_normed * gain_ref[...]
    grad_x = inv_rms * (grad_xhat - x_hat * jnp.mean(grad_xhat * x_hat, axis=-1, keepdims=True))
    out_ref[...] = (dy_ref[...].astype(jnp.float32) + grad_x).astype(jnp.bfloat16)


def epilogue(grad_normed, x_bf, dy, gain):
    tokens, dim = x_bf.shape
    rows = 64
    full = pl.BlockSpec((rows, dim), lambda i: (i, 0))
    vec = pl.BlockSpec((1, dim), lambda i: (0, 0))
    return pl.pallas_call(
        epilogue_kernel,
        grid=(tokens // rows,),
        in_specs=[full, full, full, vec],
        out_specs=[full, vec],
        out_shape=[jax.ShapeDtypeStruct((tokens, dim), jnp.bfloat16), jax.ShapeDtypeStruct((1, dim), jnp.float32)],
        cost_estimate=pl.CostEstimate(flops=tokens * dim * 1000, bytes_accessed=tokens * dim * 10, transcendentals=0),
        name="epilogue",
    )(grad_normed, x_bf, dy, gain)


def scores_t(keys, queries, mask_t, heads):
    st = lax.dot_general(keys, queries, NT, preferred_element_type=jnp.float32) * SCALE
    return jnp.where(jnp.concatenate([mask_t] * heads, axis=1), st, NEG_BIG)


def head_cols(head):
    return slice(head * HEAD_DIM, (head + 1) * HEAD_DIM)


def attn_fwd_kernel(lin_ref, cos_ref, sin_ref, qpos_ref, kpos_ref, *rest):
    o_ref, ot_ref, qkv_ref = rest[-3:]
    cos_tab, sin_tab = cos_ref[...], sin_ref[...]
    mask_t = kpos_ref[0] <= qpos_ref[0]
    rows = lin_ref.shape[0]
    rot = [rotate(lin_ref[:, head_cols(head)], cos_tab, sin_tab).astype(jnp.bfloat16) for head in range(5)]
    for head in range(5):
        qkv_ref[:, head_cols(head)] = rot[head]
    vals = lin_ref[:, head_cols(5)].astype(jnp.bfloat16)
    qkv_ref[:, head_cols(5)] = vals
    for first in (0, 2):
        st = scores_t(rot[4], jnp.concatenate(rot[first:first + 2], axis=0), mask_t, 2)
        row_max = jnp.max(st, axis=0, keepdims=True)
        probs = jnp.exp(st - row_max)
        row_sum = jnp.sum(probs, axis=0, keepdims=True)
        out_t = lax.dot_general(vals, probs.astype(jnp.bfloat16), TN, preferred_element_type=jnp.float32) / row_sum
        for i in range(2):
            part = out_t[:, i * rows:(i + 1) * rows]
            ot_ref[head_cols(first + i), :] = part.astype(jnp.bfloat16)
            o_ref[:, head_cols(first + i)] = part.T.astype(jnp.bfloat16)


def attn_bwd_kernel(qkv_ref, do_ref, o_ref, cos_ref, sin_ref, qpos_ref, kpos_ref, out_ref):
    cos_tab, sin_tab = cos_ref[...], sin_ref[...]
    mask_t = kpos_ref[0] <= qpos_ref[0]
    rows = qkv_ref.shape[0]
    keys, vals = qkv_ref[:, head_cols(4)], qkv_ref[:, head_cols(5)]
    grad_k, grad_v = [], []
    for first in (0, 2):
        pair = [head_cols(first), head_cols(first + 1)]
        queries = jnp.concatenate([qkv_ref[:, c] for c in pair], axis=0)
        gout = jnp.concatenate([do_ref[:, c] for c in pair], axis=0)
        delta = jnp.concatenate([jnp.sum((do_ref[:, c].astype(jnp.float32) * o_ref[:, c].astype(jnp.float32)).T, axis=0, keepdims=True) for c in pair], axis=1)
        st = scores_t(keys, queries, mask_t, 2)
        row_max = jnp.max(st, axis=0, keepdims=True)
        probs = jnp.exp(st - row_max)
        probs = probs * (1.0 / jnp.sum(probs, axis=0, keepdims=True))
        grad_p = lax.dot_general(vals, gout, NT, preferred_element_type=jnp.float32)
        grad_s = (probs * (grad_p - delta)).astype(jnp.bfloat16)
        grad_v.append(jnp.dot(probs.astype(jnp.bfloat16), gout, preferred_element_type=jnp.float32))
        grad_k.append(jnp.dot(grad_s, queries, preferred_element_type=jnp.float32))
        grad_qt = lax.dot_general(keys, grad_s, TN, preferred_element_type=jnp.float32)
        for i in range(2):
            grad_q = grad_qt[:, i * rows:(i + 1) * rows].T * SCALE
            out_ref[:, pair[i]] = rotate_back(grad_q, cos_tab, sin_tab).astype(jnp.bfloat16)
    out_ref[:, head_cols(4)] = rotate_back((grad_k[0] + grad_k[1]) * SCALE, cos_tab, sin_tab).astype(jnp.bfloat16)
    out_ref[:, head_cols(5)] = (grad_v[0] + grad_v[1]).astype(jnp.bfloat16)


def attn_specs(rows, first):
    packed = pl.BlockSpec((rows, GROUP), lambda b, g: (b, g))
    wide = pl.BlockSpec((rows, 4 * HEAD_DIM), lambda b, g: (b, first + g))
    tab = pl.BlockSpec((rows, HEAD_DIM), lambda b, g: (b, 0))
    qpos = pl.BlockSpec((1, 1, rows), lambda b, g: (b, 0, 0))
    kpos = pl.BlockSpec((1, rows, 1), lambda b, g: (b, 0, 0))
    return packed, wide, tab, qpos, kpos


def attn_fwd(first, lin, q_cols, tables, n_seq, prev):
    tokens, cols = lin.shape
    rows = tokens // n_seq
    packed, wide, tab, qpos, kpos = attn_specs(rows, first)
    return pl.pallas_call(
        attn_fwd_kernel,
        grid=(n_seq, cols // GROUP),
        in_specs=[packed, tab, tab, qpos, kpos] + [pl.BlockSpec(memory_space=pl.ANY)] * len(prev),
        out_specs=[wide, pl.BlockSpec((4 * HEAD_DIM, rows), lambda b, g: (first + g, b)), packed],
        out_shape=[jax.ShapeDtypeStruct((tokens, q_cols), jnp.bfloat16), jax.ShapeDtypeStruct((q_cols, tokens), jnp.bfloat16), jax.ShapeDtypeStruct((tokens, cols), jnp.bfloat16)],
        input_output_aliases={5 + i: i for i in range(len(prev))},
        cost_estimate=pl.CostEstimate(flops=cols * 5 * 10 ** 6, bytes_accessed=tokens * cols * 10, transcendentals=tokens * cols),
        compiler_params=pltpu.CompilerParams(dimension_semantics=("arbitrary", "arbitrary")),
        name="attn_fwd",
    )(lin, *tables, *prev)


def attn_bwd(first, qkv, gout, attn, tables, n_seq):
    tokens, cols = qkv.shape
    rows = tokens // n_seq
    packed, wide, tab, qpos, kpos = attn_specs(rows, first)
    return pl.pallas_call(
        attn_bwd_kernel,
        grid=(n_seq, cols // GROUP),
        in_specs=[packed, wide, wide, tab, tab, qpos, kpos],
        out_specs=packed,
        out_shape=jax.ShapeDtypeStruct((tokens, cols), jnp.bfloat16),
        cost_estimate=pl.CostEstimate(flops=cols * 10 ** 7, bytes_accessed=tokens * cols * 10, transcendentals=tokens * cols),
        compiler_params=pltpu.CompilerParams(dimension_semantics=("arbitrary", "arbitrary")),
        name="attn_bwd",
    )(qkv, gout, attn, *tables)


def dw_kernel(n_lhs, n_rhs, first, *refs):
    ids, lhs, rhs = refs[:n_lhs], refs[n_lhs:2 * n_lhs], refs[2 * n_lhs:2 * n_lhs + n_rhs]
    send_ref, keep_ref, lhs_buf, rhs_buf, lhs_sem, rhs_sem = refs[2 * n_lhs + n_rhs:]
    nblk = 2 * send_ref.shape[0]
    tile = send_ref.shape[2]
    step, steps = pl.program_id(0), pl.num_programs(0)

    def rhs_copies(at):
        cols = pl.ds(pl.multiple_of((first + at) * tile, tile), tile)
        slot = lax.rem(at, 2)
        tokens = rhs[0].shape[0]
        return [pltpu.make_async_copy(src.at[:, cols], rhs_buf.at[slot, pl.ds(i * tokens, tokens), :], rhs_sem.at[slot]) for i, src in enumerate(rhs)]

    @pl.when(step == 0)
    def _():
        for copy in rhs_copies(0):
            copy.start()
        copies = []
        for blk in range(nblk):
            col = 0
            for idx, src in zip(ids, lhs):
                depth = src.shape[1]
                start = pl.multiple_of(idx[blk] * BLK, BLK)
                copies.append(pltpu.make_async_copy(src.at[pl.ds(start, BLK), :], lhs_buf.at[pl.ds(blk * BLK, BLK), pl.ds(col, depth)], lhs_sem))
                col += depth
        for copy in copies:
            copy.start()
        for copy in copies:
            copy.wait()

    @pl.when(step + 1 < steps)
    def _():
        for copy in rhs_copies(step + 1):
            copy.start()

    for copy in rhs_copies(step):
        copy.wait()
    out = jnp.dot(lhs_buf[...], rhs_buf[lax.rem(step, 2)], preferred_element_type=jnp.float32)
    half = nblk * BLK // 2
    send_ref[...] = out[:half].reshape(send_ref.shape)
    keep_ref[...] = out[half:].reshape(keep_ref.shape)


def dw_blocks(ids, lhs, rhs, col0, ncols):
    nblk = ids[0].shape[0]
    tile = BLK
    depth = sum(part.shape[1] for part in lhs)
    out_spec = pl.BlockSpec((nblk // 2, BLK, tile), lambda j, *_: (0, 0, j))
    out_shape = jax.ShapeDtypeStruct((nblk // 2, BLK, ncols), jnp.float32)
    grid_spec = pltpu.PrefetchScalarGridSpec(
        num_scalar_prefetch=len(lhs),
        grid=(ncols // tile,),
        in_specs=[pl.BlockSpec(memory_space=pl.ANY)] * (len(lhs) + len(rhs)),
        out_specs=[out_spec, out_spec],
        scratch_shapes=[pltpu.VMEM((nblk * BLK, depth), jnp.bfloat16), pltpu.VMEM((2, depth, tile), jnp.bfloat16), pltpu.SemaphoreType.DMA, pltpu.SemaphoreType.DMA((2,))],
    )
    return pl.pallas_call(
        functools.partial(dw_kernel, len(lhs), len(rhs), col0 // tile),
        grid_spec=grid_spec,
        out_shape=[out_shape, out_shape],
        cost_estimate=pl.CostEstimate(flops=2 * nblk * BLK * depth * ncols, bytes_accessed=nblk * BLK * ncols * 4 + 2 * depth * ncols + 2 * nblk * BLK * depth, transcendentals=0),
        compiler_params=pltpu.CompilerParams(dimension_semantics=("arbitrary",)),
        name="dw",
    )(*ids, *lhs, *rhs)


def pack_kernel(q_ref, k_ref, v_ref, out_ref):
    out_ref[:, :4 * HEAD_DIM] = q_ref[...]
    out_ref[:, head_cols(4)] = k_ref[...]
    out_ref[:, head_cols(5)] = v_ref[...]


def pack_weights(first, size, w_query, w_key, w_value):
    rows = w_query.shape[0]
    kv_spec = pl.BlockSpec((rows, HEAD_DIM), lambda g: (0, first + g))
    return pl.pallas_call(
        pack_kernel,
        grid=(size,),
        in_specs=[pl.BlockSpec((rows, 4 * HEAD_DIM), lambda g: (0, first + g)), kv_spec, kv_spec],
        out_specs=pl.BlockSpec((rows, GROUP), lambda g: (0, g)),
        out_shape=jax.ShapeDtypeStruct((rows, size * GROUP), jnp.bfloat16),
        cost_estimate=pl.CostEstimate(flops=10 ** 9, bytes_accessed=4 * rows * size * GROUP, transcendentals=0),
        name="pack_weights",
    )(w_query, w_key, w_value)


def finish_qkv_kernel(keep_ref, recv_ref, last_ref, *rest):
    q_ref, k_ref, v_ref = rest[-3:]
    total = keep_ref[0] + recv_ref[0] + last_ref[...]
    q_ref[...] = total[:, :4 * HEAD_DIM]
    k_ref[...] = total[:, head_cols(4)]
    v_ref[...] = total[:, head_cols(5)]


def finish_qkv(first, keep, recv, last, q_cols, kv_cols, prev):
    part = pl.BlockSpec((1, BLK, GROUP), lambda g: (0, 0, g))
    kv_spec = pl.BlockSpec((BLK, HEAD_DIM), lambda g: (0, first + g))
    kv_out = jax.ShapeDtypeStruct((BLK, kv_cols), jnp.float32)
    return tuple(pl.pallas_call(
        finish_qkv_kernel,
        grid=(last.shape[1] // GROUP,),
        in_specs=[part, part, pl.BlockSpec((BLK, GROUP), lambda g: (0, g))] + [pl.BlockSpec(memory_space=pl.ANY)] * len(prev),
        out_specs=[pl.BlockSpec((BLK, 4 * HEAD_DIM), lambda g: (0, first + g)), kv_spec, kv_spec],
        out_shape=[jax.ShapeDtypeStruct((BLK, q_cols), jnp.float32), kv_out, kv_out],
        input_output_aliases={3 + i: i for i in range(len(prev))},
        cost_estimate=pl.CostEstimate(flops=10 ** 9, bytes_accessed=16 * last.size, transcendentals=0),
        name="finish_qkv",
    )(keep, recv, last, *prev))


WO_PIECES = (('xzy', 0, 1536), ('zxy', 1536, 1536), ('yxz', 3072, 1024))


def solution(mesh):
    fsdp_size, cp_size = mesh.shape['fsdp'], mesh.shape['cp']

    def swap(val, axis):
        if axis == 'z':
            return lax.ppermute(val, 'cp', [(i, i ^ 1) for i in range(cp_size)])
        bit = {'core': 1, 'x': 2, 'y': 4}[axis]
        return lax.ppermute(val, 'fsdp', [(i, i ^ bit) for i in range(fsdp_size)])

    def tie(val, *others):
        return lax.optimization_barrier((val,) + others)[0]

    def pick(val, idx, axis):
        return lax.dynamic_index_in_dim(val, idx, axis, False)

    def ordered(low, mine, other, axis):
        return jnp.concatenate([jnp.where(low, mine, other), jnp.where(low, other, mine)], axis=axis)

    def block_step(hidden, tok_pos, grad_out, norm_gain, w_query, w_key, w_value, w_out):
        n_all, n_rows, dim = hidden.shape
        n_seq = n_all // 2
        tokens = n_seq * 2 * n_rows
        q_cols, kv_cols = w_query.shape[1], w_key.shape[1]
        fsdp, z_idx = lax.axis_index('fsdp'), lax.axis_index('cp')
        y_idx, x_idx, core = fsdp // 4, fsdp // 2 % 2, fsdp % 2
        z_low = z_idx == 0

        gain = norm_gain.reshape(-1, 128)
        for axis, idx in (('z', z_idx), ('core', core), ('x', x_idx), ('y', y_idx)):
            other = swap(gain, axis)
            gain = ordered(idx == 0, gain, other, 0)
        gain = gain.reshape(1, dim)

        starts = [sum(CHUNKS[:i]) for i in range(len(CHUNKS))]
        w_mine, w_other = [], []
        for i, (first, size) in enumerate(zip(starts, CHUNKS)):
            w_mine.append(pack_weights(first, size, w_query, w_key, w_value))
            w_other.append(swap(w_mine[i], 'z'))

        def whole_seqs(val):
            halves = val.reshape((2, n_seq) + val.shape[1:])
            other = swap(pick(halves, 1 - z_idx, 0), 'z')
            return lambda *after: jnp.concatenate([pick(halves, z_idx, 0), tie(other, *after)], axis=1)

        def rows_back(val):
            split = val.reshape(n_seq, 2, n_rows, dim)
            other = swap(split[:, 1], 'z')
            return lambda after: ordered(z_low, split[:, 0], tie(other, after), 0)

        pos = whole_seqs(tok_pos)()
        x_bf = whole_seqs(hidden)().reshape(tokens, dim)
        dy_whole = whole_seqs(grad_out)

        half = HEAD_DIM // 2
        inv_freq = ROPE_THETA ** (-jnp.arange(half, dtype=jnp.float32) / half)
        angles = pos.reshape(tokens, 1).astype(jnp.float32) * inv_freq
        cos_tab = jnp.concatenate([jnp.cos(angles)] * 2, axis=1)
        sin_tab = jnp.concatenate([-jnp.sin(angles), jnp.sin(angles)], axis=1)
        tables = (cos_tab, sin_tab, pos.reshape(n_seq, 1, 2 * n_rows), pos.reshape(n_seq, 2 * n_rows, 1))

        def core_half(mat_t):
            other = pick(mat_t.reshape(4, 2, 2 * BLK, tokens), 1 - core, 1)
            return swap(other.reshape(-1, tokens), 'core')

        normed, normed_t = prep(x_bf, gain)
        w_full = []
        for i in range(len(CHUNKS)):
            pair = ordered(z_low, w_mine[i], w_other[i] if i == 0 else tie(w_other[i], normed), 0)
            w_full.append(lax.all_gather(pair, 'fsdp', axis=0, tiled=True))
        wo_full = lax.all_gather(w_out, ALL_AXES, axis=0, tiled=True)
        normed_tp = core_half(normed_t)
        send_own = pick(pick(normed_t.reshape(2, 2, 2, 2, BLK, tokens), core, 2), 1 - y_idx, 0)
        send_prt = pick(normed_tp.reshape(2, 2, 2, BLK, tokens), 1 - y_idx, 0)
        normed_ty = swap(jnp.concatenate([send_own, send_prt], axis=-1).reshape(4 * BLK, 2 * tokens), 'y')
        out = ()
        qkv = []
        for i, first in enumerate(starts):
            normed_now = tie(normed, *out)
            lin = jnp.dot(normed_now, w_full[i], preferred_element_type=jnp.float32)
            *out, part = attn_fwd(first, lin, q_cols, tables, n_seq, tuple(out))
            qkv.append(part)
            if i == len(CHUNKS) - 2:
                dy = dy_whole(*out).reshape(tokens, dim)
                dy_prt = swap(dy, 'core')
        attn, attn_t = out
        attn_tp = core_half(attn_t)

        own16 = fsdp * 2 + z_idx
        bits = {'y': 8, 'x': 4, 'z': 1}

        def wo_ids(order):
            flips = [bits[order[0]] * a + bits[order[1]] * b + bits[order[2]] * c for a in (1, 0) for b in (0, 1) for c in (0, 1)]
            blks = own16 ^ jnp.array(flips, jnp.int32)
            return blks, blks // 4 * 2 + blks % 2

        wo_sent, wo_keep = [], []
        for order, col0, ncols in WO_PIECES:
            rhs = (dy, tie(dy_prt, *wo_keep[-1:]))
            send, keep = dw_blocks(wo_ids(order), (attn_t, attn_tp), rhs, col0, ncols)
            wo_sent.append(swap(send, order[0]))
            wo_keep.append(keep)

        dy_now = tie(dy, *wo_keep)
        gout = lax.dot_general(dy_now, wo_full, NT, preferred_element_type=jnp.float32).astype(jnp.bfloat16)
        grads, cores, ys = [], [], []
        for i, first in enumerate(starts):
            qkv_now = qkv[i] if i == 0 else tie(qkv[i], grads[-1])
            part = attn_bwd(first, qkv_now, gout, attn, tables, n_seq)
            cores.append(swap(part, 'core'))
            ys.append(swap(part, 'y'))
            grads.append(part)

        wo_keep = [tie(keep, grads[-1]) for keep in wo_keep]
        wo_sent2 = []
        for (order, _, _), keep, recv in zip(WO_PIECES, wo_keep, wo_sent):
            wo_sent2.append(swap(keep[2:4] + recv[2:4], order[1]))
        attn_now = tie(attn, grads[-1])
        result = (x_bf.astype(jnp.float32) + jnp.dot(attn_now, wo_full, preferred_element_type=jnp.float32)).astype(jnp.bfloat16)
        result_out = rows_back(result)

        x_bits = x_idx ^ jnp.array([1, 1, 0, 0], jnp.int32)
        z_bits = z_idx ^ jnp.array([0, 1, 0, 1], jnp.int32)
        xz = x_bits * 2 + z_bits
        qkv_ids = (y_idx * 8 + x_bits * 4 + core * 2 + z_bits, y_idx * 4 + xz, xz)
        dr = None
        grad_hidden = None

        def dr_part(i, after):
            grad_now = tie(grads[i], after)
            part = lax.dot_general(grad_now, w_full[i], NT, preferred_element_type=jnp.float32)
            return part if dr is None else dr + part

        def dw_part(i, after):
            y_now = tie(ys[i], kept[-1][0] if kept else result)
            ycore = swap(y_now, 'core')
            lhs_now = (normed_t, tie(normed_tp, after), normed_ty)
            send, keep = dw_blocks(qkv_ids, lhs_now, (grads[i], cores[i], y_now, ycore), 0, grads[i].shape[1])
            return keep, swap(send, 'x')

        kept = []
        dr = dr_part(0, result)
        kept.append(dw_part(0, dr))
        dr = dr_part(1, kept[0][0])
        dr = dr_part(2, kept[0][0])
        kept.append(dw_part(1, dr))
        dr = dr_part(3, kept[1][0])
        grad_hidden, gain_grad = epilogue(dr, x_bf, dy, gain)
        grad_hidden_out = rows_back(grad_hidden)
        kept.append(dw_part(2, grad_hidden))
        kept.append(dw_part(3, kept[2][0]))

        send2, sent2 = [], []
        for i, (keep, recv) in enumerate(kept):
            keep = tie(keep, kept[-1][0], *send2[-1:])
            send2.append(keep[1] + recv[1])
            sent2.append(swap(send2[i], 'z'))

        cur = gain_grad.reshape(2, 2, 2, 2, 2, 128)
        for step, (axis, dim_at, idx) in enumerate((('x', 1, x_idx), ('y', 0, y_idx), ('core', 0, core), ('z', 0, z_idx))):
            moved = swap(pick(cur, 1 - idx, dim_at), axis)
            cur = tie(pick(cur, idx, dim_at), send2[step]) + moved
        gain_grad = cur.reshape(-1)

        wo_out = []
        for (order, _, _), keep, recv, recv2 in zip(WO_PIECES, wo_keep, wo_sent, wo_sent2):
            recv3 = swap(tie(keep, kept[1][0])[1] + recv[1] + recv2[1], order[2])
            wo_out.append(keep[0] + recv[0] + recv2[0] + recv3)
        grad_wo = jnp.concatenate(wo_out, axis=1)

        outs = ()
        for i, ((keep, recv), recv2) in enumerate(zip(kept, sent2)):
            outs = finish_qkv(starts[i], keep, recv, recv2, q_cols, kv_cols, outs)
        grad_wq, grad_wk, grad_wv = outs
        return result_out(kept[-1][0]), grad_hidden_out(send2[-1]), grad_wq, grad_wk, grad_wv, grad_wo, gain_grad

    row_spec = P('fsdp', 'cp', None)
    pos_spec = P('fsdp', 'cp')
    weight_spec = P(ALL_AXES, None)
    gain_spec = P(ALL_AXES)
    return jax.shard_map(block_step, mesh=mesh, in_specs=(row_spec, pos_spec, row_spec, gain_spec, weight_spec, weight_spec, weight_spec, weight_spec), out_specs=(row_spec, row_spec, weight_spec, weight_spec, weight_spec, weight_spec, gain_spec), check_vma=False)
```
